256 devices in a mesh: rep: 2 (over core), dp: 128 (over x, y, z).
Axes of the slice: x: 4, y: 4, z: 8, core: 2. Of those that a mesh axis runs over, the one named last changes fastest.
Arguments:
- x: bfloat16 [256, 2048, 1024], P(('rep', 'dp')), parts along dimension 0
- dy: bfloat16 [256, 2048, 1024], P(('rep', 'dp')), parts along dimension 0
- w_gate: bfloat16 [2, 1024, 3584], P(None, 'dp')
- w_up: bfloat16 [2, 1024, 3584], P(None, 'dp')
- w_down: bfloat16 [2, 3584, 1024], P(None, 'dp')
Outputs:
- output 1: bfloat16 [256, 2048, 1024], P(('rep', 'dp')), parts along dimension 0
- output 2: bfloat16 [4, 1024, 3584], P('rep', 'dp'), parts along dimension 0
- output 3: bfloat16 [4, 1024, 3584], P('rep', 'dp'), parts along dimension 0
- output 4: bfloat16 [4, 3584, 1024], P('rep', 'dp'), parts along dimension 0
There are 2 independent parts. The reference program is written for one: setup_inputs(seed, part) draws one part's arguments, and reference() takes and returns one part's arrays. A program takes and returns all parts, laid end to end along the dimension named above; an argument that names none is the same for every part.
All inputs are finite; a program needn't handle non-finite values.
Results may differ from the reference program's by a relative error of at most 0.018.
Values are sent between devices in bfloat16 or wider.
A program may use at most 768 MiB of HBM per device.

```python
import jax
import jax.numpy as jnp
from jax import lax

SEQUENCES = 128
TOKENS = 2048
D = 1024
FF = 3584
LAYERS = 2
NAMES = ("w_gate", "w_up", "w_down")
SHAPES = {"w_gate": (LAYERS, D, FF), "w_up": (LAYERS, D, FF), "w_down": (LAYERS, FF, D)}


def bump(key, n, height):
    away = (jnp.arange(n, dtype=jnp.int32) - jax.random.randint(key, (), 0, n, jnp.int32)) % n
    return jnp.where(away < n // 8, height, 1.0)


def together(key, own, strength):
    shared = jax.random.normal(key, own.shape[1:], jnp.float32)
    return (own + strength * shared) * lax.rsqrt(1 + strength * strength)


def setup_inputs(seed: int = 0, part: int = 0) -> dict:
    kx, kdy, ka, kb, kz, kf, kh, kl, *kw = jax.random.split(jax.random.key(seed), 8 + len(NAMES))
    kx, kdy, ka, kb = (jax.random.fold_in(k, part) for k in (kx, kdy, ka, kb))
    shape = (SEQUENCES, TOKENS, D)
    much_x, much_dy = jax.random.uniform(kz, (2,), jnp.float32, 0.0, 1.0)
    layers = 2.0 ** jax.random.uniform(kl, (LAYERS, 1, 1), jnp.float32, -1.0, 1.0)
    x = together(ka, jax.random.normal(kx, shape, jnp.float32), much_x) * bump(kf, D, 4.0)
    dy = together(kb, jax.random.normal(kdy, shape, jnp.float32), much_dy)
    drawn = {"x": x.astype(jnp.bfloat16), "dy": (dy * (SEQUENCES * TOKENS) ** -0.5).astype(jnp.bfloat16)}
    for key, name in zip(kw, NAMES, strict=True):
        w = jax.random.normal(key, SHAPES[name], jnp.float32) * SHAPES[name][1] ** -0.5
        drawn[name] = (w * {"w_gate": 1.0, "w_up": bump(kh, FF, 4.0), "w_down": layers}[name]).astype(jnp.bfloat16)
    return drawn


def matmul(a, w):
    return jnp.dot(a, w, preferred_element_type=jnp.float32).astype(jnp.bfloat16)


def normed(h):
    wide = h.astype(jnp.float32)
    scale = lax.rsqrt(jnp.mean(wide**2, -1, keepdims=True) + 1e-6)
    return (wide * scale).astype(jnp.bfloat16)


def layer(h, w):
    a = normed(h)
    gate = jnp.dot(a, w["w_gate"], preferred_element_type=jnp.float32)
    up = jnp.dot(a, w["w_up"], preferred_element_type=jnp.float32)
    return h + matmul((jax.nn.silu(gate) * up).astype(jnp.bfloat16), w["w_down"])


def stack(weights, h):
    return lax.scan(lambda h, w: (layer(h, w), None), h, weights)[0]


def reference(x, dy, w_gate, w_up, w_down):
    weights = dict(zip(NAMES, (w_gate, w_up, w_down), strict=True))

    def take(so_far, sequence):
        h, by_y = sequence
        _, back = jax.vjp(stack, weights, h)
        by_weights, by_h = back(by_y)
        return jax.tree.map(lambda total, term: total + term.astype(jnp.float32), so_far, by_weights), by_h

    none_yet = {name: jnp.zeros(w.shape, jnp.float32) for name, w in weights.items()}
    by_weights, by_x = lax.scan(take, none_yet, (x, dy))
    return (by_x, *(by_weights[name].astype(jnp.bfloat16) for name in NAMES))
```

```python
import jax
import jax.numpy as jnp
from jax import lax
from jax.experimental import pallas as pl
from jax.experimental.pallas import tpu as pltpu
from jax.sharding import PartitionSpec as P

T, D, FF, L = 2048, 1024, 3584, 2
X, Y, Z = 4, 4, 8
C, NC = 512, 7
H, LANES = C // 2, 128
TM = 1024
HT = TM // 2
BOTH = range(2)
NR = T // TM
PER = NR + 2
bf16, f32 = jnp.bfloat16, jnp.float32
UNITS = L * NC
SIZE = {"x": X, "y": Y, "z": Z}
RS_AXES = (("x", "y", "z"), ("y", "x", "z"), ("z", "x", "y"))
AG_AXES = tuple(tuple(reversed(a)) for a in RS_AXES)
HALVES = (((128, C), (2, 64, C), (64, C)), ((32, C), (32, C), (16, C)))
GU_PLACE = (4, 6, 9, 10, 13, 16)
PLACE = (GU_PLACE, GU_PLACE, (3, 4, 6, 8, 10, 12, 14, 16))
GU_TICK = (0, 2, 3, 5, 7, 8)
TICK = (GU_TICK, GU_TICK, (0, 1, 3, 4, 5, 6, 7, 8))
G1 = 9
G2 = G1 + NR * NC + NR
G3 = G2 + PER * NC
G4 = G3 + PER * NC
GEND = G4 + 13
LATE = 2
AG_SLOTS, SEMS = 5, 19
MESH = pl.DeviceIdType.MESH


def rs_stages(m):
    return [(p, k) for p in (0, 1) for k in range(1, SIZE[RS_AXES[m][p]] // 2 + 1)] + [(2, 1)]


def ag_stages(m):
    return [(0, 1), (1, 1)] + [(2, k) for k in range(1, SIZE[AG_AXES[m][2]] // 2 + 1)] + [(3, 1)]


def dot(a, b, ca=1, cb=0):
    return lax.dot_general(a, b, (((ca,), (cb,)), ((), ())), preferred_element_type=f32)


def rows(start, size):
    return pl.ds(start if isinstance(start, int) else pl.multiple_of(start, size), size)


def parts(n, size):
    return lax.div(n, size), lax.rem(n, size)


def norm_rows(h):
    wide = h.astype(f32)
    scale = lax.rsqrt(jnp.mean(wide * wide, -1, keepdims=True) + 1e-6)
    return (wide * scale).astype(bf16)


def norm_back(h, da):
    wide, da = h.astype(f32), da.astype(f32)
    scale = lax.rsqrt(jnp.mean(wide * wide, -1, keepdims=True) + 1e-6)
    along = jnp.sum(da * wide, -1, keepdims=True)
    return (da * scale - wide * (along * (scale * scale * scale) * (1.0 / D))).astype(bf16)


def kernel(x_hbm, dy_hbm, gate_hbm, up_hbm, down_hbm,
           dx_hbm, og_hbm, ou_hbm, od_hbm, wg_hbm, wu_hbm, wd_hbm, a0_hbm, gu_hbm, late_hbm,
           a, dy, h, acc, wg, wu, wd, act, dg, du, gst, ust, ug, uu, ud,
           halves, fulls, zb, r3, res, raw, sw, quarter, outd, half, dbuf,
           isem, wsem, gsem, lsem, ags, agr, rss, rsr, psem):
    rep, dp = lax.axis_index("rep"), lax.axis_index("dp")
    mx, left = parts(dp, Y * Z)
    my, mz = parts(left, Z)
    zp, zh = parts(mz, 2)
    me = {"x": mx, "y": my, "z": mz}
    stride = {"x": Y * Z, "y": Z, "z": 1}
    ring = {axis: [lax.rem(me[axis] + o, n) for o in range(n)] for axis, n in SIZE.items()}
    peer = {axis: [{"dp": dp + (v - me[axis]) * stride[axis]} for v in vs] for axis, vs in ring.items()}
    partner = {"rep": 1 - rep}
    twin = {"dp": dp + 1 - 2 * zh}

    def coord(axis, offset):
        return ring[axis][offset % SIZE[axis]]

    def near(axis, offset):
        return peer[axis][offset % SIZE[axis]]

    def remote(src, dst, ssem, rsem, device):
        return pltpu.make_async_remote_copy(src, dst, ssem, rsem, device_id=device, device_id_type=MESH)

    barrier = pltpu.get_barrier_semaphore()
    everyone = [partner] + [d for axis in SIZE for d in peer[axis][1:]]
    for device in everyone:
        pl.semaphore_signal(barrier, inc=1, device_id=device, device_id_type=MESH)

    def my_columns(side):
        return rows(C * side + H * rep, H)

    cx = pltpu.make_async_copy(x_hbm, h, isem.at[0])
    cdy = pltpu.make_async_copy(dy_hbm, dy, isem.at[1])
    ca0 = pltpu.make_async_copy(a, a0_hbm, isem.at[5])
    ca = pltpu.make_async_copy(a0_hbm, a, isem.at[2])
    cdx = pltpu.make_async_copy(dy, dx_hbm, isem.at[1])
    loads = [pltpu.make_async_copy(gate_hbm, raw.at[0], isem.at[2]), pltpu.make_async_copy(up_hbm, raw.at[1], isem.at[3]),
             pltpu.make_async_copy(down_hbm.at[:, :, my_columns(zh)], quarter.at[0], isem.at[4])]
    own = [
        pltpu.make_async_copy(sw.at[0], wg_hbm.at[:, rep, mx, rows(64 * my + 8 * mz, 8)], isem.at[2]),
        pltpu.make_async_copy(sw.at[1], wu_hbm.at[:, rep, mx, rows(64 * my + 8 * mz, 8)], isem.at[3]),
        pltpu.make_async_copy(sw.at[2], wd_hbm.at[:, zh, rep, rows(128 * zp + 32 * mx + 8 * my, 8)], isem.at[4]),
    ]
    swap = remote(down_hbm.at[:, :, my_columns(1 - zh)], quarter.at[1], psem.at[0, 0], psem.at[1, 0], twin)

    group = lax.shift_right_logical(lax.broadcasted_iota(jnp.int32, (8, 128), 1), 3)

    def arrange(n, _):
        l, q = parts(n, NC * 2)
        j, e = parts(q, 2)
        w = 8 * (7 * (2 * rep + e) + j)
        for m in BOTH:
            out = jnp.zeros((8, LANES), f32)
            for xy in range(X * Y):
                at = 224 * xy + w
                lanes = pltpu.roll(raw[m, l, :, rows(lax.shift_right_logical(at, 7) * LANES, LANES)].astype(f32),
                                   (8 * xy - at) & 127, 1)
                out = jnp.where(group == xy, lanes, out)
            sw[m, l * NC + j, :, rows(LANES * e, LANES)] = out.astype(bf16)
        return 0

    def begin():
        for c in loads:
            c.start()
        cx.start()
        cdy.start()
        for c in loads:
            c.wait()
        lax.fori_loop(0, UNITS, arrange, 0)
        pl.semaphore_wait(barrier, len(everyone))
        swap.start()
        lax.fori_loop(UNITS, UNITS * 2, arrange, 0)
        for c in own[:2]:
            c.start()
        swap.wait()
        for l in range(L):
            for side in BOTH:
                @pl.when(zh == side)
                def _():
                    for b in BOTH:
                        dbuf[pl.ds(28 * (side ^ b), 28), :H] = quarter[b, l].astype(f32)
            for j in range(NC):
                sw[2, l * NC + j] = dbuf[8 * j:8 * j + 8, :H].astype(bf16)
        own[2].start()

    begin()

    def ag_block(m, u, p, v, side):
        def some(start, n):
            return rows(start, n) if side is None else rows(start + n // 2 * side, n // 2)
        if m == 2:
            if p == 0:
                return wd_hbm.at[u, zh, rep, rows(128 * zp + 32 * mx + 8 * v, 8)]
            if p == 1:
                return wd_hbm.at[u, zh, rep, rows(128 * zp + 32 * v, 32)]
            pair, odd = parts(v, 2)
            return wd_hbm.at[u, odd, rep, some(128 * pair, 128)]
        w = (wg_hbm, wu_hbm)[m]
        if p == 0:
            return w.at[u, rep, mx, rows(64 * my + 8 * v, 8)]
        if m == 0:
            return w.at[u, rep, mx, rows(64 * v, 64)] if p == 1 else w.at[u, rep, v, some(0, 256)]
        if p == 1:
            return w.at[u, rep, v, rows(64 * my, 64)]
        return w.at[u, rep, some(0, X), rows(64 * v, 64)]

    def ag_copies(m, u, s):
        slot = lax.rem(u, AG_SLOTS)
        p, k = ag_stages(m)[s]

        def sems(n):
            return ags.at[slot, m, n], agr.at[slot, m, n]
        if p == 3:
            ref = (wg_hbm.at[u, rep], wu_hbm.at[u, rep], wd_hbm.at[u, :, rep])[m]
            return [remote(ref, ref, *sems(SEMS - 1), partner)]
        axis = AG_AXES[m][p]
        if p < 2:
            ref = ag_block(m, u, p, me[axis], None)
            return [remote(sw.at[m, u] if p == 0 else ref, ref, *sems(7 * p + o - 1), near(axis, o))
                    for o in range(1, SIZE[axis])]
        out = []
        for d, sign in enumerate((1, -1)):
            ref = ag_block(m, u, p, coord(axis, -sign * (k - 1)), d if k == SIZE[axis] // 2 else None)
            out.append(remote(ref, ref, *sems(8 + 2 * k + d), near(axis, sign)))
        return out

    def ag_stage(u, here):
        for m, s in here:
            if s > 0:
                for c in ag_copies(m, u, s - 1):
                    c.wait()
        for m, s in here:
            if s < len(ag_stages(m)):
                for c in ag_copies(m, u, s):
                    c.start()

    def ag_tick(t):
        for parity in BOTH:
            @pl.when(lax.rem(t, 2) == parity)
            def _():
                for at in range(parity, G1, 2):
                    here = [(m, s) for m in range(3) for s, place in enumerate(TICK[m]) if place == at]

                    @pl.when((t >= at) & (t < at + 2 * UNITS))
                    def _():
                        ag_stage(lax.div(t - at, 2), here)

    def rs_region(m, i, p, v, side):
        slot = lax.rem(i, 3)

        def some(start, n):
            return rows(start, n) if side is None else rows(start + n // 2 * side, n // 2)
        if p == 2:
            return zb[m].at[lax.rem(i, 2), v]
        if m == 0:
            return ug.at[slot, some(256 * v, 256) if p == 0 else some(256 * mx + 64 * v, 64)]
        if m == 1:
            return uu.at[slot, some(0, X), rows(64 * v, 64)] if p == 0 else uu.at[slot, v, some(64 * my, 64)]
        if p == 0:
            pair, odd = parts(v, 2)
            return ud.at[slot, some(128 * pair, 128), rows(C * odd, C)]
        return ud.at[slot, some(128 * zp + 32 * v, 32), rows(C * zh, C)]

    def rs_landing(m, i, p, k, d):
        slot = lax.rem(i, 2)
        if p == 2:
            return r3[m].at[slot, d]
        return halves[p][m].at[slot, d] if k == 1 else fulls[p][m].at[slot, k - 2, d]

    def rs_copies(m, i, s):
        p, k = rs_stages(m)[s]
        axis = RS_AXES[m][p]
        slot = lax.rem(i, 2)

        def copy(v, side, d, n, device):
            return remote(rs_region(m, i, p, v, side), rs_landing(m, i, p, k, d), rss.at[slot, m, n], rsr.at[slot, m, n], device)
        if p == 2:
            return [copy(coord(axis, o), None, o - 1, 11 + o, near(axis, o)) for o in range(1, SIZE[axis])]
        return [copy(coord(axis, sign * (SIZE[axis] // 2 + 1 - k)), d if k == 1 else None, d, 2 * s + d, near(axis, sign))
                for d, sign in enumerate((1, -1))]

    def add_tiles(dst, srcs, put):
        *lead, n, _ = dst.shape
        t = min(n, 64)
        count = (lead[0] if lead else 1) * (n // t)

        def tile(q):
            b, r = parts(q, n // t)
            ix = (b, rows(r * t, t)) if lead else (rows(q * t, t),)
            put(ix, sum((ref[ix].astype(f32) for ref in srcs), dst[ix].astype(f32)))
        if count == 1:
            tile(0)
        else:
            lax.fori_loop(0, count, lambda q, _: (tile(q), 0)[1], 0)

    def rs_stage(m, i, s):
        todo = rs_stages(m)
        if s > 0:
            for c in rs_copies(m, i, s - 1):
                c.wait()
            p, k = todo[s - 1]
            axis = RS_AXES[m][p]
            n = SIZE[axis]
            if p == 2:
                total = zb[m][lax.rem(i, 2), me[axis]].astype(f32)
                for o in range(n - 1):
                    total += r3[m][lax.rem(i, 2), o].astype(f32)
                res[m, i] = total.astype(bf16)
            elif k < n // 2:
                for d, sign in enumerate((1, -1)):
                    reg = rs_region(m, i, p, coord(axis, sign * (n // 2 - k)), d if k == 1 else None)

                    def put(ix, v, reg=reg):
                        reg[ix] = v.astype(bf16)
                    add_tiles(reg, [rs_landing(m, i, p, k, d)], put)
            else:
                mine = rs_region(m, i, p, me[axis], None)

                def put(ix, v):
                    if p == 0:
                        mine[ix] = v.astype(bf16)
                    else:
                        last = SIZE[RS_AXES[m][2]]
                        zb[m][lax.rem(i, 2)] = v.reshape(last, 8, C).astype(bf16)
                add_tiles(mine, [rs_landing(m, i, p, k, d) for d in BOTH], put)
        if s < len(todo):
            for c in rs_copies(m, i, s):
                c.start()

    def rs_hook(i, sub):
        for at in range(PER):
            @pl.when(sub == at)
            def _():
                for back in range(4, -1, -1):
                    here = [(m, s) for m in range(3) for s, place in enumerate(PLACE[m]) if place == at + PER * back]
                    if here:
                        @pl.when((i >= back) & (i < back + UNITS))
                        def _():
                            for m, s in here:
                                rs_stage(m, i - back, s)

    def send_half(l):
        return remote(half.at[0, l], half.at[1, l], psem.at[0, 1 + l], psem.at[1, 1 + l], twin)

    def collect(l):
        i0 = (L - 1 - l) * NC

        def tile(m, _):
            for t in range(FF // LANES):
                out = jnp.zeros((8, LANES), f32)
                for q in range(X * Y):
                    xy, w = divmod(16 * t + q, 28)
                    quad, j = divmod(w, NC)
                    lanes = pltpu.roll(res[m, i0 + j, :, LANES * quad:LANES * (quad + 1)].astype(f32), (8 * q - 8 * xy) % LANES, 1)
                    out = jnp.where(group == q, lanes, out)
                raw[m, l, :, LANES * t:LANES * (t + 1)] = out.astype(bf16)
            return 0
        for j in range(NC):
            dbuf[8 * j:8 * j + 8, :] = res[2, i0 + j].astype(f32)
        for side in BOTH:
            @pl.when(zh == side)
            def _():
                half[0, l] = dbuf[28 - 28 * side:56 - 28 * side, :].astype(bf16)
                outd[l, :, C * side:C * side + C] = dbuf[28 * side:28 * side + 28, :].astype(bf16)
        send_half(l).start()
        lax.fori_loop(0, 2, tile, 0)

    def w_copies(u, slot, down):
        if down:
            return [pltpu.make_async_copy(wd_hbm.at[u, q, c], wd.at[slot, :, pl.ds(C * q + H * c, H)], wsem.at[slot, 2])
                    for q in BOTH for c in BOTH]
        return [pltpu.make_async_copy(far.at[u, c], ref.at[slot, :, :, pl.ds(H * c, H)], wsem.at[slot, b])
                for b, (far, ref) in enumerate(((wg_hbm, wg), (wu_hbm, wu))) for c in BOTH]

    def w_start(u, slot, down):
        for c in w_copies(u, slot, down):
            c.start()

    def w_wait(slot, down):
        for b, ref in ((2, wd),) if down else ((0, wg), (1, wu)):
            pltpu.make_async_copy(ref.at[slot], ref.at[slot], wsem.at[slot, b]).wait()

    def gate_up(slot):
        return wg[slot].reshape(D, C), wu[slot].reshape(D, C)

    def gu_copies(n, back):
        slot = lax.rem(n, 2)
        j, r = parts(n, NR)
        out = []
        for b, st in enumerate((gst, ust)):
            far = gu_hbm.at[j, b, rows(r * TM, TM)]
            out.append(pltpu.make_async_copy(*((far, st.at[slot]) if back else (st.at[slot], far)), gsem.at[slot, b]))
        return out

    def add_da(rs, dgb, dub, slot):
        wgs, wus = gate_up(slot)
        acc[rs, :] += dot(dgb, wgs, 1, 1) + dot(dub, wus, 1, 1)

    def back_rows(gates, ups, halves_, slot, da):
        dacts = [dot(dy[rs, :], wd[slot], 1, 1).astype(bf16) for rs in halves_]
        for gate, up, dact, rs in zip(gates, ups, dacts, halves_):
            g, u, dact = gate[...], up[...], dact.astype(f32)
            sig = 1.0 / (1.0 + jnp.exp(-g))
            sl = g * sig
            act[rs, :] = (sl * u).astype(bf16)
            dub = (dact * sl).astype(bf16)
            dgb = (dact * u * (sig + sl * (1.0 - sig))).astype(bf16)
            du[rs, :] = dub
            dg[rs, :] = dgb
            if da:
                add_da(rs, dgb, dub, slot)

    def kept_rows(st):
        return [[ref.at[st, q * HT:q * HT + HT] for q in BOTH] for ref in (gst, ust)]

    def late_copies(back):
        pairs = [(v, late_hbm.at[b]) for b, v in enumerate((dg, du))]
        return [pltpu.make_async_copy(*(p[::-1] if back else p), lsem.at[b]) for b, p in enumerate(pairs)]

    def tiles(f):
        lax.fori_loop(0, T // 256, lambda q, _: (f(rows(q * 256, 256)), 0)[1], 0)

    def clear(rs):
        acc[rs, :] = jnp.zeros((256, D), f32)

    def enter(rs, new):
        h[rs, :] = new
        a[rs, :] = norm_rows(new)
        clear(rs)

    def leave(rs):
        dy[rs, :] = dy[rs, :] + norm_back(h[rs, :], acc[rs, :].astype(bf16))
        clear(rs)

    def step(g, _):
        backward = g >= G2
        i, sub = parts(jnp.maximum(g - G2, 0), PER)
        j1, r1 = parts(g + 1, NR)
        cc = jnp.where(backward, NC + i, j1 - (G1 + 1) // NR)
        r = jnp.where(backward, sub, r1)
        slot = lax.rem(cc + 2 * NC, 2)
        n1 = g - G1
        rs = rows(lax.rem(r, NR) * TM, TM)
        quarters = [rows(lax.rem(r, NR) * TM + q * HT, HT) for q in BOTH]

        @pl.when((g < G2 - NR) | (backward & (g < 2 * UNITS + G1)))
        def _():
            @pl.when(g == 1)
            def _():
                for c in own:
                    c.wait()
            with jax.named_scope("gather"):
                ag_tick(jnp.where(backward, g - NR, g))

        @pl.when(r == 0)
        def _():
            @pl.when(g == 1)
            def _():
                cx.wait()
                tiles(lambda rs: enter(rs, h[rs, :]))
                ca0.start()

            @pl.when(g == G1 + NR)
            def _():
                tiles(clear)

            @pl.when(g == G2)
            def _():
                for n in range(NC * NR - 2, NC * NR):
                    for c in gu_copies(n, False):
                        c.wait()
                ca0.wait()
                cdy.wait()
                with jax.named_scope("enter"):
                    tiles(lambda rs: enter(rs, h[rs, :] + acc[rs, :].astype(bf16)))

            @pl.when(g == G3)
            def _():
                ca.start()
                for c in gu_copies(0, True):
                    c.start()
                with jax.named_scope("leave"):
                    tiles(leave)
                cx.start()

            @pl.when((g < G4) & (cc >= 0))
            def _():
                with jax.named_scope("weights"):
                    @pl.when((cc < NC) | backward)
                    def _():
                        w_wait(slot, False)

                    @pl.when(backward)
                    def _():
                        w_wait(slot, True)

                    @pl.when((cc > 0) & (g < G2))
                    def _():
                        w_wait(1 - slot, True)

        @pl.when((r == 1) & (cc >= -1) & (cc < 3 * NC))
        def _():
            nxt = cc + 1

            @pl.when((cc < 3 * NC - 1) & ((cc < NC) | backward))
            def _():
                w_start(jnp.where(nxt < UNITS, nxt, nxt - UNITS), 1 - slot, False)

            @pl.when((cc < 3 * NC - 1) & backward)
            def _():
                w_start(jnp.where(nxt < UNITS, nxt, nxt - UNITS), 1 - slot, True)

            @pl.when((cc >= 0) & (g < G2))
            def _():
                w_start(cc, slot, True)

        @pl.when((n1 >= 0) & (g < G2))
        def _():
            st = lax.rem(n1, 2)

            @pl.when((n1 >= 2) & (n1 < NC * NR))
            def _():
                for c in gu_copies(n1 - 2, False):
                    c.wait()

            @pl.when(cc < NC)
            def _():
                with jax.named_scope("row1"):
                    ar = a[rs, :]
                    wgs, wus = gate_up(slot)
                    gst[st] = dot(ar, wgs)
                    ust[st] = dot(ar, wus)
                    acc[rs, :] += dot(act[rs, :], wd[1 - slot])
                    gate = gst[st]
                    sig = 1.0 / (1.0 + jnp.exp(-gate))
                    act[rs, :] = (gate * sig * ust[st]).astype(bf16)
                for c in gu_copies(n1, False):
                    c.start()

            @pl.when(cc == NC)
            def _():
                acc[rs, :] += dot(act[rs, :], wd[1 - slot])

        @pl.when(backward)
        def _():
            with jax.named_scope("scatter"):
                rs_hook(i, sub)
            mine = lax.rem(i, 3)

            @pl.when((sub < NR) & (g < G3))
            def _():
                with jax.named_scope("row2"):
                    wgs, wus = gate_up(slot)
                    gst[0] = dot(a[rs, :], wgs)
                    ust[0] = dot(a[rs, :], wus)
                    back_rows(*kept_rows(0), quarters, slot, True)

            @pl.when((sub < NR) & (g >= G3) & (g < G4))
            def _():
                n = (i - NC) * NR + sub
                for c in gu_copies(n, True):
                    c.wait()

                @pl.when(n + 1 < NC * NR)
                def _():
                    for c in gu_copies(n + 1, True):
                        c.start()
                kept = kept_rows(lax.rem(n, 2))

                @pl.when(i < UNITS - LATE)
                def _():
                    with jax.named_scope("row3"):
                        back_rows(*kept, quarters, slot, True)

                @pl.when((i >= UNITS - LATE) & (n == NR * (NC - 1)))
                def _():
                    for c in late_copies(False):
                        c.wait()

                @pl.when(i >= UNITS - LATE)
                def _():
                    with jax.named_scope("row3late"):
                        back_rows(*kept, quarters, slot, False)

            @pl.when((sub == NR) & (g < G4))
            def _():
                @pl.when(g == G3 + NR)
                def _():
                    ca.wait()

                @pl.when(i == UNITS - LATE)
                def _():
                    for c in late_copies(False):
                        c.start()
                with jax.named_scope("dd"):
                    ud[mine] = dot(act[...], dy[...], 0, 0).astype(bf16)

            @pl.when((sub == NR + 1) & (g < G4))
            def _():
                with jax.named_scope("dw"):
                    ug[mine] = dot(a[...], dg[...], 0, 0).astype(bf16)
                    uu[mine] = dot(a[...], du[...], 0, 0).astype(bf16).reshape(X, H, C)

            @pl.when(g >= G4)
            def _():
                n = g - G4

                @pl.when(n == NR + 1)
                def _():
                    for c in late_copies(True):
                        c.wait()

                @pl.when((n < NR) | ((n > NR) & (n <= 2 * NR)))
                def _():
                    late, q = parts(n, NR + 1)
                    rs = rows(q * TM, TM)
                    with jax.named_scope("late"):
                        add_da(rs, dg[rs, :], du[rs, :], late)

                @pl.when(n == NR - 1)
                def _():
                    for c in late_copies(True):
                        c.start()

                @pl.when(n == NR)
                def _():
                    cx.wait()

                @pl.when((n == NR) | (g == GEND - 1))
                def _():
                    with jax.named_scope("collect"):
                        collect(jnp.where(n == NR, 1, 0))

                @pl.when(n == 2 * NR + 1)
                def _():
                    tiles(leave)
                    cdx.start()
        return 0

    lax.fori_loop(0, GEND, step, 0)
    ends = [pltpu.make_async_copy(raw.at[0], og_hbm, isem.at[2]), pltpu.make_async_copy(raw.at[1], ou_hbm, isem.at[3]),
            pltpu.make_async_copy(outd, od_hbm, isem.at[4])]
    for c in ends[:2]:
        c.start()
    for l in range(L):
        send_half(l).wait()
        outd[l, :, rows(C * (1 - zh), C)] = half[1, l]
    ends[2].start()
    for c in ends:
        c.wait()
    cdx.wait()


def mega(x, dy, gate, up, down):
    S = jax.ShapeDtypeStruct
    V = pltpu.VMEM
    DMA = pltpu.SemaphoreType.DMA
    hbm = pl.BlockSpec(memory_space=pl.ANY)
    outs = [S((T, D), bf16), S((L, 8, FF), bf16), S((L, 8, FF), bf16), S((L, 28, D), bf16),
            *[S((UNITS, 2, X, H, H), bf16)] * 2, S((UNITS, 2, 2, C, H), bf16),
            S((T, D), bf16), S((NC, 2, T, C), f32), S((2, T, C), bf16)]
    scratch = [
        *[V((T, D), bf16)] * 3, V((T, D), f32),
        *[V((2, X, H, C), bf16)] * 2, V((2, C, D), bf16),
        *[V((T, C), bf16)] * 3, *[V((2, TM, C), f32)] * 2,
        V((3, D, C), bf16), V((3, X, H, C), bf16), V((3, C, D), bf16),
        tuple(tuple(V((2, 2, *s), bf16) for s in shapes) for shapes in HALVES),
        tuple(tuple(V((2, SIZE[RS_AXES[m][p]] // 2 - 1, 2, 2 * s[0], *s[1:]), bf16) for m, s in enumerate(shapes))
              for p, shapes in enumerate(HALVES)),
        tuple(V((2, SIZE[axes[2]], 8, C), bf16) for axes in RS_AXES),
        tuple(V((2, SIZE[axes[2]] - 1, 8, C), bf16) for axes in RS_AXES),
        V((3, UNITS, 8, C), bf16), V((2, L, 8, FF), bf16), V((3, UNITS, 8, H), bf16), V((2, L, 28, H), bf16),
        V((L, 28, D), bf16), V((2, L, 28, C), bf16), V((56, C), f32),
        DMA((6,)), DMA((2, 3)), DMA((2, 2)), DMA((2,)), *[DMA((AG_SLOTS, 3, SEMS))] * 2, *[DMA((2, 3, SEMS))] * 2,
        DMA((2, 3)),
    ]
    return pl.pallas_call(
        kernel, out_shape=outs, in_specs=[hbm] * 5, out_specs=[hbm] * len(outs), scratch_shapes=scratch, name="mega",
        compiler_params=pltpu.CompilerParams(collective_id=0, has_side_effects=True, vmem_limit_bytes=67043328),
    )(x, dy, gate, up, down)[:4]


def body(x, dy, *weights):
    dx, *by_weights = mega(x[0], dy[0], *weights)
    return (dx[None], *by_weights)


def solution(mesh):
    rows_, seq, grad = P(None, "dp", None), P(("rep", "dp"), None, None), P("rep", "dp", None)
    return jax.shard_map(body, mesh=mesh, in_specs=(seq, seq, rows_, rows_, rows_),
                         out_specs=(seq, grad, grad, grad), check_vma=False)
```

```python
import jax
import jax.numpy as jnp
from jax import lax
from jax.experimental import pallas as pl
from jax.experimental.pallas import tpu as pltpu
from jax.sharding import PartitionSpec as P

T, D, FF, L = 2048, 1024, 3584, 2
X, Y, Z = 4, 4, 8
C, NC = 512, 7
H, LANES = C // 2, 128
TM = 1024
HT = TM // 2
BOTH, MATRICES = range(2), range(3)
NR = T // TM
PER = NR + 2
bf16, f32 = jnp.bfloat16, jnp.float32
UNITS = L * NC
SIZE = {"x": X, "y": Y, "z": Z}
RS_AXES = (("x", "y", "z"), ("y", "x", "z"), ("z", "x", "y"))
AG_AXES = tuple(tuple(reversed(a)) for a in RS_AXES)
HALVES = (((128, C), (2, 64, C), (64, C)), ((32, C), (32, C), (16, C)))
GU_PLACE = (4, 6, 9, 11, 13, 16)
PLACE = (GU_PLACE, GU_PLACE, (3, 4, 7, 9, 11, 12, 14, 16))
GU_TICK = (0, 2, 3, 5, 7, 8)
TICK = (GU_TICK, GU_TICK, (0, 1, 3, 4, 5, 6, 7, 8))
G1 = 9
G2 = G1 + NR * NC + NR
G3 = G2 + PER * NC
G4 = G3 + PER * NC
GEND = G4 + 13
LATE = 4
AG_SLOTS, SEMS = 5, 19
MESH = pl.DeviceIdType.MESH


def rs_stages(m):
    return [(p, k) for p in (0, 1) for k in range(1, SIZE[RS_AXES[m][p]] // 2 + 1)] + [(2, 1)]


def ag_stages(m):
    return [(0, 1), (1, 1)] + [(2, k) for k in range(1, SIZE[AG_AXES[m][2]] // 2 + 1)] + [(3, 1)]


def odd_of(n):
    return lax.rem(n, 2)


def dot(a, b, ca=1, cb=0):
    return lax.dot_general(a, b, (((ca,), (cb,)), ((), ())), preferred_element_type=f32)


def rows(start, size):
    return pl.ds(start if isinstance(start, int) else pl.multiple_of(start, size), size)


def parts(n, size):
    return lax.div(n, size), lax.rem(n, size)


def rms_scale(wide):
    return lax.rsqrt(jnp.mean(wide * wide, -1, keepdims=True) + 1e-6)


def norm_rows(h):
    wide = h.astype(f32)
    return (wide * rms_scale(wide)).astype(bf16)


def norm_back(h, da):
    wide, da = h.astype(f32), da.astype(f32)
    scale = rms_scale(wide)
    along = jnp.sum(da * wide, -1, keepdims=True)
    return (da * scale - wide * (along * (scale * scale * scale) * (1.0 / D))).astype(bf16)


def kernel(x_hbm, dy_hbm, gate_hbm, up_hbm, down_hbm,
           dx_hbm, og_hbm, ou_hbm, od_hbm, wg_hbm, wu_hbm, wd_hbm, a0_hbm, gu_hbm, late_hbm,
           a, dy, h, acc, wg, wu, wd, act, dg, du, gst, ust, ug, uu, ud,
           halves, fulls, zb, r3, res, raw, sw, quarter, outd, half, dbuf,
           isem, wsem, gsem, lsem, ags, agr, rss, rsr, psem):
    rep, dp = lax.axis_index("rep"), lax.axis_index("dp")
    mx, left = parts(dp, Y * Z)
    my, mz = parts(left, Z)
    zp, zh = parts(mz, 2)
    me = {"x": mx, "y": my, "z": mz}
    stride = {"x": Y * Z, "y": Z, "z": 1}
    ring = {axis: [lax.rem(me[axis] + o, n) for o in range(n)] for axis, n in SIZE.items()}
    peer = {axis: [{"dp": dp + (v - me[axis]) * stride[axis]} for v in vs] for axis, vs in ring.items()}
    partner = {"rep": 1 - rep}
    twin = {"dp": dp + 1 - 2 * zh}

    def coord(axis, offset):
        return ring[axis][offset % SIZE[axis]]

    def near(axis, offset):
        return peer[axis][offset % SIZE[axis]]

    def remote(src, dst, ssem, rsem, device):
        return pltpu.make_async_remote_copy(src, dst, ssem, rsem, device_id=device, device_id_type=MESH)

    barrier = pltpu.get_barrier_semaphore()
    everyone = [partner] + [d for axis in SIZE for d in peer[axis][1:]]
    for device in everyone:
        pl.semaphore_signal(barrier, inc=1, device_id=device, device_id_type=MESH)

    def my_columns(side):
        return rows(C * side + H * rep, H)

    cx = pltpu.make_async_copy(x_hbm, h, isem.at[0])
    cdy = pltpu.make_async_copy(dy_hbm, dy, isem.at[1])
    ca0 = pltpu.make_async_copy(a, a0_hbm, isem.at[5])
    ca = pltpu.make_async_copy(a0_hbm, a, isem.at[2])
    cdx = pltpu.make_async_copy(dy, dx_hbm, isem.at[1])
    loads = [pltpu.make_async_copy(gate_hbm, raw.at[0], isem.at[2]), pltpu.make_async_copy(up_hbm, raw.at[1], isem.at[3]),
             pltpu.make_async_copy(down_hbm.at[:, :, my_columns(zh)], quarter.at[0], isem.at[4])]
    own = [
        pltpu.make_async_copy(sw.at[0], wg_hbm.at[:, rep, mx, rows(64 * my + 8 * mz, 8)], isem.at[2]),
        pltpu.make_async_copy(sw.at[1], wu_hbm.at[:, rep, mx, rows(64 * my + 8 * mz, 8)], isem.at[3]),
        pltpu.make_async_copy(sw.at[2], wd_hbm.at[:, zh, rep, rows(128 * zp + 32 * mx + 8 * my, 8)], isem.at[4]),
    ]
    swap = remote(down_hbm.at[:, :, my_columns(1 - zh)], quarter.at[1], psem.at[0, 0], psem.at[1, 0], twin)

    group = lax.shift_right_logical(lax.broadcasted_iota(jnp.int32, (8, 128), 1), 3)

    def arrange(n, _):
        l, q = parts(n, NC * 2)
        j, e = parts(q, 2)
        w = 8 * (7 * (2 * rep + e) + j)
        for m in BOTH:
            out = jnp.zeros((8, LANES), f32)
            for xy in range(X * Y):
                at = 224 * xy + w
                lanes = pltpu.roll(raw[m, l, :, rows(lax.shift_right_logical(at, 7) * LANES, LANES)].astype(f32),
                                   (8 * xy - at) & 127, 1)
                out = jnp.where(group == xy, lanes, out)
            sw[m, l * NC + j, :, rows(LANES * e, LANES)] = out.astype(bf16)
        return 0

    def ag_block(m, u, p, v, side):
        def some(start, n):
            return rows(start, n) if side is None else rows(start + n // 2 * side, n // 2)
        if m == 2:
            if p == 0:
                return wd_hbm.at[u, zh, rep, rows(128 * zp + 32 * mx + 8 * v, 8)]
            if p == 1:
                return wd_hbm.at[u, zh, rep, rows(128 * zp + 32 * v, 32)]
            pair, odd = parts(v, 2)
            return wd_hbm.at[u, odd, rep, some(128 * pair, 128)]
        w = (wg_hbm, wu_hbm)[m]
        if p == 0:
            return w.at[u, rep, mx, rows(64 * my + 8 * v, 8)]
        if m == 0:
            return w.at[u, rep, mx, rows(64 * v, 64)] if p == 1 else w.at[u, rep, v, some(0, 256)]
        if p == 1:
            return w.at[u, rep, v, rows(64 * my, 64)]
        return w.at[u, rep, some(0, X), rows(64 * v, 64)]

    def ag_copies(m, u, s):
        slot = lax.rem(u, AG_SLOTS)
        p, k = ag_stages(m)[s]

        def sems(n):
            return ags.at[slot, m, n], agr.at[slot, m, n]
        if p == 3:
            ref = (wg_hbm.at[u, rep], wu_hbm.at[u, rep], wd_hbm.at[u, :, rep])[m]
            return [remote(ref, ref, *sems(SEMS - 1), partner)]
        axis = AG_AXES[m][p]
        if p < 2:
            ref = ag_block(m, u, p, me[axis], None)
            return [remote(sw.at[m, u] if p == 0 else ref, ref, *sems(7 * p + o - 1), near(axis, o))
                    for o in range(1, SIZE[axis])]
        out = []
        for d, sign in enumerate((1, -1)):
            ref = ag_block(m, u, p, coord(axis, -sign * (k - 1)), d if k == SIZE[axis] // 2 else None)
            out.append(remote(ref, ref, *sems(8 + 2 * k + d), near(axis, sign)))
        return out

    def ag_stage(u, here):
        for m, s in here:
            if s > 0:
                for c in ag_copies(m, u, s - 1):
                    c.wait()
        for m, s in here:
            if s < len(ag_stages(m)):
                for c in ag_copies(m, u, s):
                    c.start()

    def ag_tick(t):
        for parity in BOTH:
            @pl.when(odd_of(t) == parity)
            def _():
                for at in range(parity, G1, 2):
                    here = [(m, s) for m in MATRICES for s, place in enumerate(TICK[m]) if place == at]

                    @pl.when((t >= at) & (t < at + 2 * UNITS))
                    def _():
                        ag_stage(lax.div(t - at, 2), here)

    def begin():
        def arrange_some(first, last):
            lax.fori_loop(first, last, arrange, 0)

        def send_first(*ms):
            for m in ms:
                for c in ag_copies(m, 0, 0):
                    c.start()
        for c in loads:
            c.start()
        cx.start()
        cdy.start()
        for c in loads:
            c.wait()
        arrange_some(0, 2)
        pl.semaphore_wait(barrier, len(everyone))
        swap.start()
        send_first(0, 1)
        arrange_some(2, UNITS)
        swap.wait()
        for l in range(L):
            for side in BOTH:
                @pl.when(zh == side)
                def _():
                    for b in BOTH:
                        dbuf[pl.ds(28 * (side ^ b), 28), :H] = quarter[b, l].astype(f32)
            for j in range(NC):
                sw[2, l * NC + j] = dbuf[8 * j:8 * j + 8, :H].astype(bf16)
        own[2].start()
        send_first(2)
        arrange_some(UNITS, 2 * UNITS)
        for c in own[:2]:
            c.start()
        cx.wait()
        tiles(lambda rs: enter(rs, h[rs, :]))
        ca0.start()
        for c in own:
            c.wait()
        lax.fori_loop(1, G1, lambda t, _: (ag_tick(t), 0)[1], 0)

    def rs_region(m, i, p, v, side):
        slot = lax.rem(i, 3)

        def some(start, n):
            return rows(start, n) if side is None else rows(start + n // 2 * side, n // 2)
        if p == 2:
            return zb[m].at[odd_of(i), v]
        if m == 0:
            return ug.at[slot, some(256 * v, 256) if p == 0 else some(256 * mx + 64 * v, 64)]
        if m == 1:
            return uu.at[slot, some(0, X), rows(64 * v, 64)] if p == 0 else uu.at[slot, v, some(64 * my, 64)]
        if p == 0:
            pair, odd = parts(v, 2)
            return ud.at[slot, some(128 * pair, 128), rows(C * odd, C)]
        return ud.at[slot, some(128 * zp + 32 * v, 32), rows(C * zh, C)]

    def rs_landing(m, i, p, k, d):
        slot = odd_of(i)
        if p == 2:
            return r3[m].at[slot, d]
        return halves[p][m].at[slot, d] if k == 1 else fulls[p][m].at[slot, k - 2, d]

    def rs_copies(m, i, s):
        p, k = rs_stages(m)[s]
        axis = RS_AXES[m][p]
        slot = odd_of(i)

        def copy(v, side, d, n, device):
            return remote(rs_region(m, i, p, v, side), rs_landing(m, i, p, k, d), rss.at[slot, m, n], rsr.at[slot, m, n], device)
        if p == 2:
            return [copy(coord(axis, o), None, o - 1, 11 + o, near(axis, o)) for o in range(1, SIZE[axis])]
        return [copy(coord(axis, sign * (SIZE[axis] // 2 + 1 - k)), d if k == 1 else None, d, 2 * s + d, near(axis, sign))
                for d, sign in enumerate((1, -1))]

    def add_tiles(dst, srcs, put):
        *lead, n, _ = dst.shape
        t = min(n, 64)
        count = (lead[0] if lead else 1) * (n // t)

        def tile(q):
            b, r = parts(q, n // t)
            ix = (b, rows(r * t, t)) if lead else (rows(q * t, t),)
            put(ix, sum((ref[ix].astype(f32) for ref in srcs), dst[ix].astype(f32)))
        if count == 1:
            tile(0)
        else:
            lax.fori_loop(0, count, lambda q, _: (tile(q), 0)[1], 0, unroll=True)

    def rs_stage(m, i, s):
        todo = rs_stages(m)
        if s > 0:
            for c in rs_copies(m, i, s - 1):
                c.wait()
            p, k = todo[s - 1]
            axis = RS_AXES[m][p]
            n = SIZE[axis]
            if p == 2:
                total = zb[m][odd_of(i), me[axis]].astype(f32)
                for o in range(n - 1):
                    total += r3[m][odd_of(i), o].astype(f32)
                res[m, i] = total.astype(bf16)
            elif k < n // 2:
                for d, sign in enumerate((1, -1)):
                    reg = rs_region(m, i, p, coord(axis, sign * (n // 2 - k)), d if k == 1 else None)

                    def put(ix, v, reg=reg):
                        reg[ix] = v.astype(bf16)
                    add_tiles(reg, [rs_landing(m, i, p, k, d)], put)
            else:
                mine = rs_region(m, i, p, me[axis], None)

                def put(ix, v):
                    if p == 0:
                        mine[ix] = v.astype(bf16)
                    else:
                        last = SIZE[RS_AXES[m][2]]
                        zb[m][odd_of(i)] = v.reshape(last, 8, C).astype(bf16)
                add_tiles(mine, [rs_landing(m, i, p, k, d) for d in BOTH], put)
        if s < len(todo):
            for c in rs_copies(m, i, s):
                c.start()

    def rs_hook(i, sub):
        for at in range(PER):
            @pl.when(sub == at)
            def _():
                for back in range(5)[::1 if at % 2 else -1]:
                    here = [(m, s) for m in MATRICES for s, place in enumerate(PLACE[m]) if place == at + PER * back]
                    if here:
                        @pl.when((i >= back) & (i < back + UNITS))
                        def _():
                            for m, s in here:
                                rs_stage(m, i - back, s)

    def send_half(l):
        return remote(half.at[0, l], half.at[1, l], psem.at[0, 1 + l], psem.at[1, 1 + l], twin)

    def collect(l):
        i0 = (L - 1 - l) * NC

        def tile(m, _):
            for t in range(FF // LANES):
                out = jnp.zeros((8, LANES), f32)
                for q in range(X * Y):
                    xy, w = divmod(16 * t + q, 28)
                    quad, j = divmod(w, NC)
                    lanes = pltpu.roll(res[m, i0 + j, :, LANES * quad:LANES * (quad + 1)].astype(f32), (8 * q - 8 * xy) % LANES, 1)
                    out = jnp.where(group == q, lanes, out)
                raw[m, l, :, LANES * t:LANES * (t + 1)] = out.astype(bf16)
            return 0
        for j in range(NC):
            dbuf[8 * j:8 * j + 8, :] = res[2, i0 + j].astype(f32)
        for side in BOTH:
            @pl.when(zh == side)
            def _():
                half[0, l] = dbuf[28 - 28 * side:56 - 28 * side, :].astype(bf16)
                outd[l, :, C * side:C * side + C] = dbuf[28 * side:28 * side + 28, :].astype(bf16)
        send_half(l).start()
        lax.fori_loop(0, 2, tile, 0)

    def w_copies(u, slot, down):
        if down:
            return [pltpu.make_async_copy(wd_hbm.at[u, q, c], wd.at[slot, :, pl.ds(C * q + H * c, H)], wsem.at[slot, 2])
                    for q in BOTH for c in BOTH]
        return [pltpu.make_async_copy(far.at[u, c], ref.at[slot, :, :, pl.ds(H * c, H)], wsem.at[slot, b])
                for b, (far, ref) in enumerate(((wg_hbm, wg), (wu_hbm, wu))) for c in BOTH]

    def w_start(u, slot, down):
        for c in w_copies(u, slot, down):
            c.start()

    def w_wait(slot, down):
        for b, ref in ((2, wd),) if down else ((0, wg), (1, wu)):
            pltpu.make_async_copy(ref.at[slot], ref.at[slot], wsem.at[slot, b]).wait()

    def gate_up(slot):
        return wg[slot].reshape(D, C), wu[slot].reshape(D, C)

    def gu_copies(n, back):
        slot = odd_of(n)
        j, r = parts(n, NR)
        out = []
        for b, st in enumerate((gst, ust)):
            far = gu_hbm.at[j, b, rows(r * TM, TM)]
            out.append(pltpu.make_async_copy(*((far, st.at[slot]) if back else (st.at[slot], far)), gsem.at[slot, b]))
        return out

    def add_da(rs, dgb, dub, slot):
        wgs, wus = gate_up(slot)
        acc[rs, :] += dot(dgb, wgs, 1, 1) + dot(dub, wus, 1, 1)

    def back_rows(gates, ups, halves_, slot, da):
        dacts = [dot(dy[rs, :], wd[slot], 1, 1).astype(bf16) for rs in halves_]
        for gate, up, dact, rs in zip(gates, ups, dacts, halves_):
            g, u, dact = gate[...], up[...], dact.astype(f32)
            sig = 1.0 / (1.0 + jnp.exp(-g))
            sl = g * sig
            act[rs, :] = (sl * u).astype(bf16)
            dub = (dact * sl).astype(bf16)
            dgb = (dact * u * (sig + sl * (1.0 - sig))).astype(bf16)
            du[rs, :] = dub
            dg[rs, :] = dgb
            if da:
                add_da(rs, dgb, dub, slot)

    def kept_rows(st):
        return [[ref.at[st, q * HT:q * HT + HT] for q in BOTH] for ref in (gst, ust)]

    def late_buffers(k):
        return (a.at[:, :C], a.at[:, C:]) if k % 2 else (dg, du)

    def late_copies(k, refs, back):
        pairs = [(v, late_hbm.at[k - 1, b], lsem.at[odd_of(k), b]) for b, v in enumerate(refs)]
        return [pltpu.make_async_copy(*((far, v) if back else (v, far)), sem) for v, far, sem in pairs]

    def tiles(f):
        lax.fori_loop(0, T // 256, lambda q, _: (f(rows(q * 256, 256)), 0)[1], 0)

    def clear(rs):
        acc[rs, :] = jnp.zeros((256, D), f32)

    def enter(rs, new):
        h[rs, :] = new
        a[rs, :] = norm_rows(new)
        clear(rs)

    def leave(rs):
        dy[rs, :] = dy[rs, :] + norm_back(h[rs, :], acc[rs, :].astype(bf16))
        clear(rs)

    def step(g, _):
        backward = g >= G2
        i, sub = parts(jnp.maximum(g - G2, 0), PER)
        j1, r1 = parts(g + 1, NR)
        cc = jnp.where(backward, NC + i, j1 - (G1 + 1) // NR)
        r = jnp.where(backward, sub, r1)
        slot = odd_of(cc + 2 * NC)
        n1 = g - G1
        rs = rows(lax.rem(r, NR) * TM, TM)
        quarters = [rows(lax.rem(r, NR) * TM + q * HT, HT) for q in BOTH]

        @pl.when((g < G2 - NR) | (backward & (sub < NR) & (i < NC)))
        def _():
            with jax.named_scope("gather"):
                ag_tick(jnp.where(backward, G2 - NR + NR * i + sub, g))

        @pl.when(r == 0)
        def _():
            @pl.when(g == G1 + NR)
            def _():
                tiles(clear)

            @pl.when(g == G2)
            def _():
                for n in range(NC * NR - 2, NC * NR):
                    for c in gu_copies(n, False):
                        c.wait()
                ca0.wait()
                cdy.wait()
                with jax.named_scope("enter"):
                    tiles(lambda rs: enter(rs, h[rs, :] + acc[rs, :].astype(bf16)))

            @pl.when(g == G3)
            def _():
                ca.start()
                for c in gu_copies(0, True):
                    c.start()
                with jax.named_scope("leave"):
                    tiles(leave)
                cx.start()

            @pl.when(g < G4)
            def _():
                with jax.named_scope("weights"):
                    @pl.when((cc < NC) | backward)
                    def _():
                        w_wait(slot, False)

                    @pl.when(backward)
                    def _():
                        w_wait(slot, True)

                    @pl.when((cc > 0) & (g < G2))
                    def _():
                        w_wait(1 - slot, True)

        @pl.when((r == 1) & (cc < 3 * NC))
        def _():
            nxt = cc + 1

            @pl.when((cc < 3 * NC - 1) & ((cc < NC) | backward))
            def _():
                w_start(jnp.where(nxt < UNITS, nxt, nxt - UNITS), 1 - slot, False)

            @pl.when((cc < 3 * NC - 1) & backward)
            def _():
                w_start(jnp.where(nxt < UNITS, nxt, nxt - UNITS), 1 - slot, True)

            @pl.when(g < G2)
            def _():
                w_start(cc, slot, True)

        @pl.when(g < G2)
        def _():
            st = odd_of(n1)

            @pl.when((n1 >= 2) & (n1 < NC * NR))
            def _():
                for c in gu_copies(n1 - 2, False):
                    c.wait()

            @pl.when(cc < NC)
            def _():
                with jax.named_scope("row1"):
                    ar = a[rs, :]
                    wgs, wus = gate_up(slot)
                    gst[st] = dot(ar, wgs)
                    ust[st] = dot(ar, wus)
                    acc[rs, :] += dot(act[rs, :], wd[1 - slot])
                    gate = gst[st]
                    sig = 1.0 / (1.0 + jnp.exp(-gate))
                    act[rs, :] = (gate * sig * ust[st]).astype(bf16)
                for c in gu_copies(n1, False):
                    c.start()

            @pl.when(cc == NC)
            def _():
                acc[rs, :] += dot(act[rs, :], wd[1 - slot])

        @pl.when(backward)
        def _():
            with jax.named_scope("scatter"):
                rs_hook(i, sub)
            mine = lax.rem(i, 3)

            @pl.when((sub < NR) & (g < G3))
            def _():
                with jax.named_scope("row2"):
                    wgs, wus = gate_up(slot)
                    for q, part in enumerate(quarters):
                        gst[0, q * HT:q * HT + HT] = dot(a[part, :], wgs)
                        ust[0, q * HT:q * HT + HT] = dot(a[part, :], wus)
                    back_rows(*kept_rows(0), quarters, slot, True)

            @pl.when((sub < NR) & (g >= G3) & (g < G4))
            def _():
                n = (i - NC) * NR + sub
                for c in gu_copies(n, True):
                    c.wait()

                @pl.when(n + 1 < NC * NR)
                def _():
                    for c in gu_copies(n + 1, True):
                        c.start()
                kept = kept_rows(odd_of(n))

                @pl.when(i < UNITS - LATE)
                def _():
                    with jax.named_scope("row3"):
                        back_rows(*kept, quarters, slot, True)

                @pl.when((i > UNITS - LATE) & (sub == 0))
                def _():
                    for c in late_copies(UNITS - i, (dg, du), False):
                        c.wait()

                @pl.when(i >= UNITS - LATE)
                def _():
                    with jax.named_scope("row3late"):
                        back_rows(*kept, quarters, slot, False)

            @pl.when((sub == NR) & (g < G4))
            def _():
                @pl.when(g == G3 + NR)
                def _():
                    ca.wait()

                @pl.when((i >= UNITS - LATE) & (i < UNITS - 1))
                def _():
                    for c in late_copies(UNITS - 1 - i, (dg, du), False):
                        c.start()
                with jax.named_scope("dd"):
                    ud[mine] = dot(act[...], dy[...], 0, 0).astype(bf16)

            @pl.when((sub == NR + 1) & (g < G4))
            def _():
                with jax.named_scope("dw"):
                    ug[mine] = dot(a[...], dg[...], 0, 0).astype(bf16)
                    uu[mine] = dot(a[...], du[...], 0, 0).astype(bf16).reshape(X, H, C)

            @pl.when(g >= G4)
            def _():
                n = g - G4

                k, q = parts(n, NR)
                kslot = odd_of(k)

                @pl.when(n == 0)
                def _():
                    for c in late_copies(1, late_buffers(1), True):
                        c.start()

                for odd in BOTH:
                    here = (kslot == odd) & (k < LATE)

                    @pl.when(here & (q == 0) & (k > 0))
                    def _():
                        for c in late_copies(k, late_buffers(odd), True):
                            c.wait()

                        @pl.when(k > 1)
                        def _():
                            w_wait(kslot, False)

                    @pl.when(here)
                    def _():
                        tile = rows(q * TM, TM)
                        with jax.named_scope("late"):
                            add_da(tile, *(ref[tile, :] for ref in late_buffers(odd)), kslot)

                    @pl.when(here & (q == NR - 1) & (k < LATE - 2))
                    def _():
                        for c in late_copies(k + 2, late_buffers(odd), True):
                            c.start()
                        w_start(NC - 3 - k, kslot, False)

                @pl.when(n == 0)
                def _():
                    cx.wait()

                @pl.when(g >= GEND - 2)
                def _():
                    with jax.named_scope("collect"):
                        collect(GEND - 1 - g)

                @pl.when(g == GEND - 3)
                def _():
                    tiles(leave)
                    cdx.start()
        return 0

    with jax.named_scope("begin"):
        begin()
    w_start(0, 0, False)
    lax.fori_loop(G1, GEND, step, 0)
    ends = [pltpu.make_async_copy(raw.at[0], og_hbm, isem.at[2]), pltpu.make_async_copy(raw.at[1], ou_hbm, isem.at[3]),
            pltpu.make_async_copy(outd, od_hbm, isem.at[4])]
    for c in ends[:2]:
        c.start()
    for l in range(L):
        send_half(l).wait()
        outd[l, :, rows(C * (1 - zh), C)] = half[1, l]
    ends[2].start()
    for c in ends:
        c.wait()
    cdx.wait()


def mega(x, dy, gate, up, down):
    S = jax.ShapeDtypeStruct
    V = pltpu.VMEM
    DMA = pltpu.SemaphoreType.DMA
    hbm = pl.BlockSpec(memory_space=pl.ANY)
    outs = [S((T, D), bf16), S((L, 8, FF), bf16), S((L, 8, FF), bf16), S((L, 28, D), bf16),
            *[S((UNITS, 2, X, H, H), bf16)] * 2, S((UNITS, 2, 2, C, H), bf16),
            S((T, D), bf16), S((NC, 2, T, C), f32), S((LATE - 1, 2, T, C), bf16)]
    scratch = [
        *[V((T, D), bf16)] * 3, V((T, D), f32),
        *[V((2, X, H, C), bf16)] * 2, V((2, C, D), bf16),
        *[V((T, C), bf16)] * 3, *[V((2, TM, C), f32)] * 2,
        V((3, D, C), bf16), V((3, X, H, C), bf16), V((3, C, D), bf16),
        tuple(tuple(V((2, 2, *s), bf16) for s in shapes) for shapes in HALVES),
        tuple(tuple(V((2, SIZE[RS_AXES[m][p]] // 2 - 1, 2, 2 * s[0], *s[1:]), bf16) for m, s in enumerate(shapes))
              for p, shapes in enumerate(HALVES)),
        tuple(V((2, SIZE[axes[2]], 8, C), bf16) for axes in RS_AXES),
        tuple(V((2, SIZE[axes[2]] - 1, 8, C), bf16) for axes in RS_AXES),
        V((3, UNITS, 8, C), bf16), V((2, L, 8, FF), bf16), V((3, UNITS, 8, H), bf16), V((2, L, 28, H), bf16),
        V((L, 28, D), bf16), V((2, L, 28, C), bf16), V((56, C), f32),
        DMA((6,)), DMA((2, 3)), *[DMA((2, 2))] * 2, *[DMA((AG_SLOTS, 3, SEMS))] * 2, *[DMA((2, 3, SEMS))] * 2,
        DMA((2, 3)),
    ]
    return pl.pallas_call(
        kernel, out_shape=outs, in_specs=[hbm] * 5, out_specs=[hbm] * len(outs), scratch_shapes=scratch, name="mega",
        compiler_params=pltpu.CompilerParams(collective_id=0, has_side_effects=True, vmem_limit_bytes=67043328),
    )(x, dy, gate, up, down)[:4]


def body(x, dy, *weights):
    dx, *by_weights = mega(x[0], dy[0], *weights)
    return (dx[None], *by_weights)


def solution(mesh):
    rows_, seq, grad = P(None, "dp", None), P(("rep", "dp"), None, None), P("rep", "dp", None)
    return jax.shard_map(body, mesh=mesh, in_specs=(seq, seq, rows_, rows_, rows_),
                         out_specs=(seq, grad, grad, grad), check_vma=False)
```

```python
import jax
import jax.numpy as jnp
from jax import lax
from jax.experimental import pallas as pl
from jax.experimental.pallas import tpu as pltpu
from jax.sharding import PartitionSpec as P

T, D, FF, L = 2048, 1024, 3584, 2
X, Y, Z = 4, 4, 8
C, NC = 512, 7
H, LANES, SPAN, EACH = C // 2, 128, 64, 28
TM = 1024
HT = TM // 2
BOTH, MATRICES = range(2), range(3)
NR = T // TM
PER = NR + 2
bf16, f32 = jnp.bfloat16, jnp.float32
UNITS = L * NC
SIZE = {"x": X, "y": Y, "z": Z}
RS_AXES = (("x", "y", "z"), ("y", "x", "z"), ("z", "x", "y"))
AG_AXES = tuple(tuple(reversed(a)) for a in RS_AXES)
HALVES = (((128, C), (2, 64, C), (64, C)), ((32, C), (32, C), (16, C)))
GU_PLACE = (4, 6, 9, 11, 13, 16)
PLACE = (GU_PLACE, GU_PLACE, (3, 4, 7, 9, 11, 12, 14, 16))
GU_TICK = (0, 2, 3, 5, 7, 8)
TICK = (GU_TICK, GU_TICK, tuple(t for t in range(9) if t != 2))
G1 = 9
G2 = G1 + NR * NC + NR
G3 = G2 + PER * NC
G4 = G3 + PER * NC
GEND = G4 + 13
LATE = 4
AG_SLOTS, SEMS = 5, 19
MESH = pl.DeviceIdType.MESH


def rs_stages(m):
    return [(p, k) for p in (0, 1) for k in range(1, SIZE[RS_AXES[m][p]] // 2 + 1)] + [(2, 1)]


def ag_stages(m):
    return [(0, 1), (1, 1)] + [(2, k) for k in range(1, SIZE[AG_AXES[m][2]] // 2 + 1)] + [(3, 1)]


def odd_of(n):
    return lax.rem(n, 2)


def dot(a, b, ca=1, cb=0):
    return lax.dot_general(a, b, (((ca,), (cb,)), ((), ())), preferred_element_type=f32)


def rows(start, size):
    return pl.ds(start if isinstance(start, int) else pl.multiple_of(start, size), size)


def parts(n, size):
    return lax.div(n, size), lax.rem(n, size)


def rms_scale(wide):
    return lax.rsqrt(jnp.mean(wide * wide, -1, keepdims=True) + 1e-6)


def norm_rows(h):
    wide = h.astype(f32)
    return (wide * rms_scale(wide)).astype(bf16)


def norm_back(h, da):
    wide, da = h.astype(f32), da.astype(f32)
    scale = rms_scale(wide)
    along = jnp.sum(da * wide, -1, keepdims=True)
    return (da * scale - wide * (along * (scale * scale * scale) * (1.0 / D))).astype(bf16)


def kernel(x_hbm, dy_hbm, gate_hbm, up_hbm, down_hbm,
           dx_hbm, og_hbm, ou_hbm, od_hbm, wg_hbm, wu_hbm, wd_hbm, a0_hbm, gu_hbm, late_hbm,
           a, dy, h, acc, wg, wu, wd, act, dg, du, gst, ust, ug, uu, ud,
           halves, fulls, zb, r3, res, raw, sw, quarter, outd, half, dbuf,
           isem, wsem, gsem, lsem, ags, agr, rss, rsr, psem):
    rep, dp = lax.axis_index("rep"), lax.axis_index("dp")
    mx, left = parts(dp, Y * Z)
    my, mz = parts(left, Z)
    zp, zh = parts(mz, 2)
    me = {"x": mx, "y": my, "z": mz}
    stride = {"x": Y * Z, "y": Z, "z": 1}
    ring = {axis: [lax.rem(me[axis] + o, n) for o in range(n)] for axis, n in SIZE.items()}
    peer = {axis: [{"dp": dp + (v - me[axis]) * stride[axis]} for v in vs] for axis, vs in ring.items()}
    partner = {"rep": 1 - rep}
    twin = {"dp": dp + 1 - 2 * zh}

    def coord(axis, offset):
        return ring[axis][offset % SIZE[axis]]

    def near(axis, offset):
        return peer[axis][offset % SIZE[axis]]

    def remote(src, dst, ssem, rsem, device):
        return pltpu.make_async_remote_copy(src, dst, ssem, rsem, device_id=device, device_id_type=MESH)

    barrier = pltpu.get_barrier_semaphore()
    everyone = [partner] + [d for axis in SIZE for d in peer[axis][1:]]
    for device in everyone:
        pl.semaphore_signal(barrier, inc=1, device_id=device, device_id_type=MESH)

    def my_columns(side):
        return rows(C * side + H * rep, H)

    cx = pltpu.make_async_copy(x_hbm, h, isem.at[0])
    cdy = pltpu.make_async_copy(dy_hbm, dy, isem.at[1])
    ca0 = pltpu.make_async_copy(a, a0_hbm, isem.at[5])
    ca = pltpu.make_async_copy(a0_hbm, a, isem.at[2])
    cdx = pltpu.make_async_copy(dy, dx_hbm, isem.at[1])
    loads = [pltpu.make_async_copy(gate_hbm, raw.at[0], isem.at[2]), pltpu.make_async_copy(up_hbm, raw.at[1], isem.at[3]),
             pltpu.make_async_copy(down_hbm.at[:, :, my_columns(zh)], quarter.at[0], isem.at[4])]
    own = [
        pltpu.make_async_copy(sw.at[0], wg_hbm.at[:, rep, mx, rows(SPAN * my + 8 * mz, 8)], isem.at[2]),
        pltpu.make_async_copy(sw.at[1], wu_hbm.at[:, rep, mx, rows(SPAN * my + 8 * mz, 8)], isem.at[3]),
        pltpu.make_async_copy(sw.at[2], wd_hbm.at[:, zh, rep, rows(LANES * zp + 32 * mx + 8 * my, 8)], isem.at[4]),
    ]
    swap = remote(down_hbm.at[:, :, my_columns(1 - zh)], quarter.at[1], psem.at[0, 0], psem.at[1, 0], twin)

    group = lax.shift_right_logical(lax.broadcasted_iota(jnp.int32, (8, LANES), 1), 3)

    def arrange(n, _):
        l, q = parts(n, NC * 2)
        j, e = parts(q, 2)
        w = 8 * (7 * (2 * rep + e) + j)
        for m in BOTH:
            out = jnp.zeros((8, LANES), f32)
            for xy in range(X * Y):
                at = 224 * xy + w
                lanes = pltpu.roll(raw[m, l, :, rows(lax.shift_right_logical(at, 7) * LANES, LANES)].astype(f32),
                                   (8 * xy - at) & 127, 1)
                out = jnp.where(group == xy, lanes, out)
            sw[m, l * NC + j, :, rows(LANES * e, LANES)] = out.astype(bf16)
        return 0

    def ag_block(m, u, p, v, side):
        def some(start, n):
            return rows(start, n) if side is None else rows(start + n // 2 * side, n // 2)
        if m == 2:
            if p == 0:
                return wd_hbm.at[u, zh, rep, rows(LANES * zp + 32 * mx + 8 * v, 8)]
            if p == 1:
                return wd_hbm.at[u, zh, rep, rows(LANES * zp + 32 * v, 32)]
            pair, odd = parts(v, 2)
            return wd_hbm.at[u, odd, rep, some(LANES * pair, LANES)]
        w = (wg_hbm, wu_hbm)[m]
        if p == 0:
            return w.at[u, rep, mx, rows(SPAN * my + 8 * v, 8)]
        if m == 0:
            return w.at[u, rep, mx, rows(SPAN * v, SPAN)] if p == 1 else w.at[u, rep, v, some(0, H)]
        if p == 1:
            return w.at[u, rep, v, rows(SPAN * my, SPAN)]
        return w.at[u, rep, some(0, X), rows(SPAN * v, SPAN)]

    def ag_copies(m, u, s):
        slot = lax.rem(u, AG_SLOTS)
        p, k = ag_stages(m)[s]

        def sems(n):
            return ags.at[slot, m, n], agr.at[slot, m, n]
        if p == 3:
            ref = (wg_hbm.at[u, rep], wu_hbm.at[u, rep], wd_hbm.at[u, :, rep])[m]
            return [remote(ref, ref, *sems(SEMS - 1), partner)]
        axis = AG_AXES[m][p]
        if p < 2:
            ref = ag_block(m, u, p, me[axis], None)
            return [remote(sw.at[m, u] if p == 0 else ref, ref, *sems(7 * p + o - 1), near(axis, o))
                    for o in range(1, SIZE[axis])]
        out = []
        for d, sign in enumerate((1, -1)):
            ref = ag_block(m, u, p, coord(axis, -sign * (k - 1)), d if k == SIZE[axis] // 2 else None)
            out.append(remote(ref, ref, *sems(8 + 2 * k + d), near(axis, sign)))
        return out

    def ag_stage(u, here):
        for m, s in here:
            if s > 0:
                for c in ag_copies(m, u, s - 1):
                    c.wait()
        for m, s in here:
            if s < len(ag_stages(m)):
                for c in ag_copies(m, u, s):
                    c.start()

    def ag_tick(t):
        for parity in BOTH:
            @pl.when(odd_of(t) == parity)
            def _():
                for at in range(parity, G1, 2):
                    here = [(m, s) for m in MATRICES for s, place in enumerate(TICK[m]) if place == at]

                    @pl.when((t >= at) & (t < at + 2 * UNITS))
                    def _():
                        ag_stage(lax.div(t - at, 2), here)

    def begin():
        def arrange_some(first, last):
            lax.fori_loop(first, last, arrange, 0)

        def send_first(*ms):
            for m in ms:
                for c in ag_copies(m, 0, 0):
                    c.start()
        for c in loads:
            c.start()
        cx.start()
        cdy.start()
        for c in loads:
            c.wait()
        arrange_some(0, 2)
        pl.semaphore_wait(barrier, len(everyone))
        swap.start()
        send_first(0, 1)
        arrange_some(2, UNITS)
        swap.wait()
        for l in range(L):
            for side in BOTH:
                @pl.when(zh == side)
                def _():
                    for b in BOTH:
                        dbuf[pl.ds(EACH * (side ^ b), EACH), :H] = quarter[b, l].astype(f32)
            for j in range(NC):
                sw[2, l * NC + j] = dbuf[8 * j:8 * j + 8, :H].astype(bf16)
        own[2].start()
        send_first(2)
        arrange_some(UNITS, 2 * UNITS)
        for c in own[:2]:
            c.start()
        cx.wait()
        tiles(lambda rs: enter(rs, h[rs, :]))
        ca0.start()
        for c in own:
            c.wait()
        lax.fori_loop(1, G1, lambda t, _: (ag_tick(t), 0)[1], 0)

    def rs_region(m, i, p, v, side):
        slot = lax.rem(i, 3)

        def some(start, n):
            return rows(start, n) if side is None else rows(start + n // 2 * side, n // 2)
        if p == 2:
            return zb[m].at[odd_of(i), v]
        if m == 0:
            return ug.at[slot, some(H * v, H) if p == 0 else some(H * mx + SPAN * v, SPAN)]
        if m == 1:
            return uu.at[slot, some(0, X), rows(SPAN * v, SPAN)] if p == 0 else uu.at[slot, v, some(SPAN * my, SPAN)]
        if p == 0:
            pair, odd = parts(v, 2)
            return ud.at[slot, some(LANES * pair, LANES), rows(C * odd, C)]
        return ud.at[slot, some(LANES * zp + 32 * v, 32), rows(C * zh, C)]

    def rs_landing(m, i, p, k, d):
        slot = odd_of(i)
        if p == 2:
            return r3[m].at[slot, d]
        return halves[p][m].at[slot, d] if k == 1 else fulls[p][m].at[slot, k - 2, d]

    def rs_copies(m, i, s):
        p, k = rs_stages(m)[s]
        axis = RS_AXES[m][p]
        slot = odd_of(i)

        def copy(v, side, d, n, device):
            return remote(rs_region(m, i, p, v, side), rs_landing(m, i, p, k, d), rss.at[slot, m, n], rsr.at[slot, m, n], device)
        if p == 2:
            return [copy(coord(axis, o), None, o - 1, 11 + o, near(axis, o)) for o in range(1, SIZE[axis])]
        return [copy(coord(axis, sign * (SIZE[axis] // 2 + 1 - k)), d if k == 1 else None, d, 2 * s + d, near(axis, sign))
                for d, sign in enumerate((1, -1))]

    def add_tiles(dst, srcs, put):
        *lead, n, _ = dst.shape
        t = min(n, SPAN)
        count = (lead[0] if lead else 1) * (n // t)

        def tile(q):
            b, r = parts(q, n // t)
            ix = (b, rows(r * t, t)) if lead else (rows(q * t, t),)
            put(ix, sum((ref[ix].astype(f32) for ref in srcs), dst[ix].astype(f32)))
        if count == 1:
            tile(0)
        else:
            lax.fori_loop(0, count, lambda q, _: (tile(q), 0)[1], 0, unroll=True)

    def rs_stage(m, i, s):
        todo = rs_stages(m)
        if s > 0:
            for c in rs_copies(m, i, s - 1):
                c.wait()
            p, k = todo[s - 1]
            axis = RS_AXES[m][p]
            n = SIZE[axis]
            if p == 2:
                total = zb[m][odd_of(i), me[axis]].astype(f32)
                for o in range(n - 1):
                    total += r3[m][odd_of(i), o].astype(f32)
                res[m, i] = total.astype(bf16)
            elif k < n // 2:
                for d, sign in enumerate((1, -1)):
                    reg = rs_region(m, i, p, coord(axis, sign * (n // 2 - k)), d if k == 1 else None)

                    def put(ix, v, reg=reg):
                        reg[ix] = v.astype(bf16)
                    add_tiles(reg, [rs_landing(m, i, p, k, d)], put)
            else:
                mine = rs_region(m, i, p, me[axis], None)

                def put(ix, v):
                    if p == 0:
                        mine[ix] = v.astype(bf16)
                    else:
                        last = SIZE[RS_AXES[m][2]]
                        zb[m][odd_of(i)] = v.reshape(last, 8, C).astype(bf16)
                add_tiles(mine, [rs_landing(m, i, p, k, d) for d in BOTH], put)
        if s < len(todo):
            for c in rs_copies(m, i, s):
                c.start()

    def rs_hook(i, sub):
        for at in range(PER):
            @pl.when(sub == at)
            def _():
                for back in range(5)[::1 if at % 2 else -1]:
                    here = [(m, s) for m in MATRICES for s, place in enumerate(PLACE[m]) if place == at + PER * back]
                    if here:
                        @pl.when((i >= back) & (i < back + UNITS))
                        def _():
                            for m, s in here:
                                rs_stage(m, i - back, s)

    def send_half(l):
        return remote(half.at[0, l], half.at[1, l], psem.at[0, 1 + l], psem.at[1, 1 + l], twin)

    def collect_down(l):
        i0 = (L - 1 - l) * NC
        for j in range(NC):
            dbuf[8 * j:8 * j + 8, :] = res[2, i0 + j].astype(f32)
        for side in BOTH:
            @pl.when(zh == side)
            def _():
                half[0, l] = dbuf[EACH - EACH * side:56 - EACH * side, :].astype(bf16)
                outd[l, :, C * side:C * side + C] = dbuf[EACH * side:EACH * side + EACH, :].astype(bf16)
        send_half(l).start()

    def collect(l):
        i0 = (L - 1 - l) * NC

        def tile(m, _):
            for t in range(FF // LANES):
                out = jnp.zeros((8, LANES), f32)
                for q in range(X * Y):
                    xy, w = divmod(16 * t + q, EACH)
                    quad, j = divmod(w, NC)
                    lanes = pltpu.roll(res[m, i0 + j, :, LANES * quad:LANES * (quad + 1)].astype(f32), (8 * q - 8 * xy) % LANES, 1)
                    out = jnp.where(group == q, lanes, out)
                raw[m, l, :, LANES * t:LANES * (t + 1)] = out.astype(bf16)
            return 0
        lax.fori_loop(0, 2, tile, 0)

    def w_copies(u, slot, down):
        if down:
            return [pltpu.make_async_copy(wd_hbm.at[u, q, c], wd.at[slot, :, pl.ds(C * q + H * c, H)], wsem.at[slot, 2])
                    for q in BOTH for c in BOTH]
        return [pltpu.make_async_copy(far.at[u, c], ref.at[slot, :, :, pl.ds(H * c, H)], wsem.at[slot, b])
                for b, (far, ref) in enumerate(((wg_hbm, wg), (wu_hbm, wu))) for c in BOTH]

    def w_start(u, slot, down):
        for c in w_copies(u, slot, down):
            c.start()

    def w_wait(slot, down):
        for b, ref in ((2, wd),) if down else ((0, wg), (1, wu)):
            pltpu.make_async_copy(ref.at[slot], ref.at[slot], wsem.at[slot, b]).wait()

    def gate_up(slot):
        return wg[slot].reshape(D, C), wu[slot].reshape(D, C)

    def gu_copies(n, back):
        slot = odd_of(n)
        j, r = parts(n, NR)
        out = []
        for b, st in enumerate((gst, ust)):
            far = gu_hbm.at[j, b, rows(r * TM, TM)]
            out.append(pltpu.make_async_copy(*((far, st.at[slot]) if back else (st.at[slot], far)), gsem.at[slot, b]))
        return out

    def add_da(rs, dgb, dub, slot):
        wgs, wus = gate_up(slot)
        acc[rs, :] += dot(dgb, wgs, 1, 1) + dot(dub, wus, 1, 1)

    def back_rows(gates, ups, halves_, slot, da):
        dacts = [dot(dy[rs, :], wd[slot], 1, 1).astype(bf16) for rs in halves_]
        for gate, up, dact, rs in zip(gates, ups, dacts, halves_):
            g, u, dact = gate[...], up[...], dact.astype(f32)
            sig = 1.0 / (1.0 + jnp.exp(-g))
            sl = g * sig
            act[rs, :] = (sl * u).astype(bf16)
            dub = (dact * sl).astype(bf16)
            dgb = (dact * u * (sig + sl * (1.0 - sig))).astype(bf16)
            du[rs, :] = dub
            dg[rs, :] = dgb
            if da:
                add_da(rs, dgb, dub, slot)

    def kept_rows(st):
        return [[ref.at[st, q * HT:q * HT + HT] for q in BOTH] for ref in (gst, ust)]

    def late_buffers(k):
        return (a.at[:, :C], a.at[:, C:]) if k % 2 else (dg, du)

    def late_copies(k, refs, back):
        pairs = [(v, late_hbm.at[k - 1, b], lsem.at[odd_of(k), b]) for b, v in enumerate(refs)]
        return [pltpu.make_async_copy(*((far, v) if back else (v, far)), sem) for v, far, sem in pairs]

    def tiles(f):
        lax.fori_loop(0, T // H, lambda q, _: (f(rows(q * H, H)), 0)[1], 0)

    def clear(rs):
        acc[rs, :] = jnp.zeros((H, D), f32)

    def enter(rs, new):
        h[rs, :] = new
        a[rs, :] = norm_rows(new)
        clear(rs)

    def leave(rs):
        dy[rs, :] = dy[rs, :] + norm_back(h[rs, :], acc[rs, :].astype(bf16))
        clear(rs)

    def step(g, _):
        backward = g >= G2
        i, sub = parts(jnp.maximum(g - G2, 0), PER)
        j1, r1 = parts(g + 1, NR)
        cc = jnp.where(backward, NC + i, j1 - (G1 + 1) // NR)
        r = jnp.where(backward, sub, r1)
        slot = odd_of(cc + 2 * NC)
        n1 = g - G1
        rs = rows(lax.rem(r, NR) * TM, TM)
        quarters = [rows(lax.rem(r, NR) * TM + q * HT, HT) for q in BOTH]

        @pl.when((g < G2 - NR) | (backward & (sub < NR) & (i < NC)))
        def _():
            with jax.named_scope("gather"):
                ag_tick(jnp.where(backward, G2 - NR + NR * i + sub, g))

        @pl.when(r == 0)
        def _():
            @pl.when(g == G1 + NR)
            def _():
                tiles(clear)

            @pl.when(g == G2)
            def _():
                for n in range(NC * NR - 2, NC * NR):
                    for c in gu_copies(n, False):
                        c.wait()
                ca0.wait()
                cdy.wait()
                with jax.named_scope("enter"):
                    tiles(lambda rs: enter(rs, h[rs, :] + acc[rs, :].astype(bf16)))

            @pl.when(g == G3)
            def _():
                ca.start()
                for c in gu_copies(0, True):
                    c.start()
                with jax.named_scope("leave"):
                    tiles(leave)
                cx.start()

            @pl.when(g < G4)
            def _():
                with jax.named_scope("weights"):
                    @pl.when((cc < NC) | backward)
                    def _():
                        w_wait(slot, False)

                    @pl.when(backward)
                    def _():
                        w_wait(slot, True)

                    @pl.when((cc > 0) & (g < G2))
                    def _():
                        w_wait(1 - slot, True)

        @pl.when((r == 1) & (cc < 3 * NC))
        def _():
            nxt = cc + 1

            @pl.when((cc < 3 * NC - 1) & ((cc < NC) | backward))
            def _():
                w_start(jnp.where(nxt < UNITS, nxt, nxt - UNITS), 1 - slot, False)

            @pl.when((cc < 3 * NC - 1) & backward)
            def _():
                w_start(jnp.where(nxt < UNITS, nxt, nxt - UNITS), 1 - slot, True)

            @pl.when(g < G2)
            def _():
                w_start(cc, slot, True)

        @pl.when(g < G2)
        def _():
            st = odd_of(n1)

            @pl.when((n1 >= 2) & (n1 < NC * NR))
            def _():
                for c in gu_copies(n1 - 2, False):
                    c.wait()

            @pl.when(cc < NC)
            def _():
                with jax.named_scope("row1"):
                    ar = a[rs, :]
                    wgs, wus = gate_up(slot)
                    gst[st] = dot(ar, wgs)
                    ust[st] = dot(ar, wus)
                    acc[rs, :] += dot(act[rs, :], wd[1 - slot])
                    gate = gst[st]
                    sig = 1.0 / (1.0 + jnp.exp(-gate))
                    act[rs, :] = (gate * sig * ust[st]).astype(bf16)
                for c in gu_copies(n1, False):
                    c.start()

            @pl.when(cc == NC)
            def _():
                acc[rs, :] += dot(act[rs, :], wd[1 - slot])

        @pl.when(backward)
        def _():
            with jax.named_scope("scatter"):
                rs_hook(i, sub)
            mine = lax.rem(i, 3)

            @pl.when((sub < NR) & (g < G3))
            def _():
                with jax.named_scope("row2"):
                    wgs, wus = gate_up(slot)
                    for q, part in enumerate(quarters):
                        gst[0, q * HT:q * HT + HT] = dot(a[part, :], wgs)
                        ust[0, q * HT:q * HT + HT] = dot(a[part, :], wus)
                    back_rows(*kept_rows(0), quarters, slot, True)

            @pl.when((sub < NR) & (g >= G3) & (g < G4))
            def _():
                n = (i - NC) * NR + sub
                for c in gu_copies(n, True):
                    c.wait()

                @pl.when(n + 1 < NC * NR)
                def _():
                    for c in gu_copies(n + 1, True):
                        c.start()
                kept = kept_rows(odd_of(n))

                @pl.when(i < UNITS - LATE)
                def _():
                    with jax.named_scope("row3"):
                        back_rows(*kept, quarters, slot, True)

                @pl.when((i > UNITS - LATE) & (sub == 0))
                def _():
                    for c in late_copies(UNITS - i, (dg, du), False):
                        c.wait()

                @pl.when(i >= UNITS - LATE)
                def _():
                    with jax.named_scope("row3late"):
                        back_rows(*kept, quarters, slot, False)

            @pl.when((sub == NR) & (g < G4))
            def _():
                @pl.when(g == G3 + NR)
                def _():
                    ca.wait()

                @pl.when((i >= UNITS - LATE) & (i < UNITS - 1))
                def _():
                    for c in late_copies(UNITS - 1 - i, (dg, du), False):
                        c.start()
                with jax.named_scope("dd"):
                    ud[mine] = dot(act[...], dy[...], 0, 0).astype(bf16)

            @pl.when((sub == NR + 1) & (g < G4))
            def _():
                with jax.named_scope("dw"):
                    ug[mine] = dot(a[...], dg[...], 0, 0).astype(bf16)
                    uu[mine] = dot(a[...], du[...], 0, 0).astype(bf16).reshape(X, H, C)

            @pl.when(g >= G4)
            def _():
                n = g - G4

                k, q = parts(n, NR)
                kslot = odd_of(k)

                @pl.when(n == 0)
                def _():
                    for c in late_copies(1, late_buffers(1), True):
                        c.start()

                for odd in BOTH:
                    here = (kslot == odd) & (k < LATE)

                    @pl.when(here & (q == 0) & (k > 0))
                    def _():
                        for c in late_copies(k, late_buffers(odd), True):
                            c.wait()

                        @pl.when(k > 1)
                        def _():
                            w_wait(kslot, False)

                    @pl.when(here)
                    def _():
                        tile = rows(q * TM, TM)
                        with jax.named_scope("late"):
                            add_da(tile, *(ref[tile, :] for ref in late_buffers(odd)), kslot)

                    @pl.when(here & (q == NR - 1) & (k < LATE - 2))
                    def _():
                        for c in late_copies(k + 2, late_buffers(odd), True):
                            c.start()
                        w_start(NC - 3 - k, kslot, False)

                @pl.when(n == 0)
                def _():
                    cx.wait()

                @pl.when(g >= GEND - 2)
                def _():
                    with jax.named_scope("collect"):
                        collect_down(GEND - 1 - g)
                        collect(GEND - 1 - g)

                @pl.when(g == GEND - 3)
                def _():
                    tiles(leave)
                    cdx.start()
        return 0

    with jax.named_scope("begin"):
        begin()
    w_start(0, 0, False)
    lax.fori_loop(G1, GEND, step, 0)
    ends = [pltpu.make_async_copy(raw.at[0], og_hbm, isem.at[2]), pltpu.make_async_copy(raw.at[1], ou_hbm, isem.at[3]),
            pltpu.make_async_copy(outd, od_hbm, isem.at[4])]
    for c in ends[:2]:
        c.start()
    for l in range(L):
        send_half(l).wait()
        outd[l, :, rows(C * (1 - zh), C)] = half[1, l]
    ends[2].start()
    for c in ends:
        c.wait()
    cdx.wait()


def mega(x, dy, gate, up, down):
    S = jax.ShapeDtypeStruct
    V = pltpu.VMEM
    DMA = pltpu.SemaphoreType.DMA
    hbm = pl.BlockSpec(memory_space=pl.ANY)
    outs = [S((T, D), bf16), S((L, 8, FF), bf16), S((L, 8, FF), bf16), S((L, EACH, D), bf16),
            *[S((UNITS, 2, X, H, H), bf16)] * 2, S((UNITS, 2, 2, C, H), bf16),
            S((T, D), bf16), S((NC, 2, T, C), f32), S((LATE - 1, 2, T, C), bf16)]
    scratch = [
        *[V((T, D), bf16)] * 3, V((T, D), f32),
        *[V((2, X, H, C), bf16)] * 2, V((2, C, D), bf16),
        *[V((T, C), bf16)] * 3, *[V((2, TM, C), f32)] * 2,
        V((3, D, C), bf16), V((3, X, H, C), bf16), V((3, C, D), bf16),
        tuple(tuple(V((2, 2, *s), bf16) for s in shapes) for shapes in HALVES),
        tuple(tuple(V((2, SIZE[RS_AXES[m][p]] // 2 - 1, 2, 2 * s[0], *s[1:]), bf16) for m, s in enumerate(shapes))
              for p, shapes in enumerate(HALVES)),
        tuple(V((2, SIZE[axes[2]], 8, C), bf16) for axes in RS_AXES),
        tuple(V((2, SIZE[axes[2]] - 1, 8, C), bf16) for axes in RS_AXES),
        V((3, UNITS, 8, C), bf16), V((2, L, 8, FF), bf16), V((3, UNITS, 8, H), bf16), V((2, L, EACH, H), bf16),
        V((L, EACH, D), bf16), V((2, L, EACH, C), bf16), V((56, C), f32),
        DMA((6,)), DMA((2, 3)), *[DMA((2, 2))] * 2, *[DMA((AG_SLOTS, 3, SEMS))] * 2, *[DMA((2, 3, SEMS))] * 2,
        DMA((2, 3)),
    ]
    return pl.pallas_call(
        kernel, out_shape=outs, in_specs=[hbm] * 5, out_specs=[hbm] * len(outs), scratch_shapes=scratch, name="mega",
        compiler_params=pltpu.CompilerParams(collective_id=0, has_side_effects=True, vmem_limit_bytes=67043328),
    )(x, dy, gate, up, down)[:4]


def hand_over(*arrays):
    k, n = len(arrays), 8

    def move(*refs):
        ins, outs, kept, sems = refs[:k], refs[k:-k - 1], refs[-k - 1:-1], refs[-1]
        first, *others = zip(ins, kept, outs)
        steps = [[ref.at[pl.ds(q * T // n, T // n)] for ref in first] for q in range(n)] + others
        reads, writes = ([pltpu.make_async_copy(*step[b:b + 2], sems.at[b, q]) for q, step in enumerate(steps)] for b in BOTH)
        for c in reads:
            c.start()
        for c, d in zip(reads, writes):
            c.wait()
            d.start()
        for d in writes:
            d.wait()
    hbm = [pl.BlockSpec(memory_space=pl.ANY)] * k
    like = [jax.ShapeDtypeStruct(t.shape, t.dtype) for t in arrays]
    return pl.pallas_call(
        move, out_shape=like, in_specs=hbm, out_specs=hbm, name="hand_over",
        scratch_shapes=[pltpu.VMEM(t.shape, t.dtype) for t in like] + [pltpu.SemaphoreType.DMA((2, n + k))],
    )(*arrays)


def body(x, dy, *weights):
    dx, gate, up, down = mega(x[0], dy[0], *weights)
    dx, gate, up = hand_over(dx, gate, up)
    return dx[None], gate, up, down


def solution(mesh):
    rows_, seq, grad = P(None, "dp", None), P(("rep", "dp"), None, None), P("rep", "dp", None)
    return jax.shard_map(body, mesh=mesh, in_specs=(seq, seq, rows_, rows_, rows_),
                         out_specs=(seq, grad, grad, grad), check_vma=False)
```
